32 devices in a mesh: tile: 8 (over y, x, core), bulk: 4 (over z).
Axes of the slice: x: 2, y: 2, z: 4, core: 2. Of those that a mesh axis runs over, the one named last changes fastest.
Arguments:
- integrals: bfloat16 [96, 256, 768], P(('tile', 'bulk')), may hold values from -0.21875 to 0.21875
- amplitudes: bfloat16 [4, 768, 1024], P(None, 'bulk', 'tile'), may hold values from -6 to 6
- residual_in: bfloat16 [96, 256, 1024], P(('tile', 'bulk')), may hold values from -6 to 6
- tile_irrep: int32 [96], replicated, may hold values from 0 to 3, as said below
Outputs:
- residual: bfloat16 [96, 256, 1024], P(('tile', 'bulk'))
The draws below stay inside these ranges and needn't reach their ends.
Inputs may be any that keep to these rules, and one draw needn't show every extreme that they name: tile_irrep never falls along the tiles, and every irrep labels at least 12 tiles.
All inputs are finite; a program needn't handle non-finite values.
Results may differ from the reference program's by a relative error of at most 0.001.
Values may be sent and summed in bfloat16 or wider, within the bound.
A program may use at most 64 MiB of HBM per device.

```python
import jax
import jax.numpy as jnp
from jax import lax

V = 768
PP = 1024
IRREPS = 4
TILE = 256
ROW_TILES = 12
NT = 96


def draw_tile_irrep(key, part):
    spare_tiles = NT - 4 * ROW_TILES
    cut_points = jnp.sort(jax.random.randint(key, (3,), 0, spare_tiles + 1))
    bounds = cut_points.astype(jnp.int32) + ROW_TILES * jnp.arange(1, 4, dtype=jnp.int32)
    positions = jnp.arange(NT, dtype=jnp.int32)
    return jnp.sum((positions[:, None] >= bounds[None, :]).astype(jnp.int32), axis=1).astype(jnp.int32)


def block_levels(key, dims, shards, smallest, largest):
    factor_of = 1.0
    for position, blocks in shards:
        steps = jax.random.uniform(jax.random.fold_in(jax.random.fold_in(key, 6), position), (blocks,), jnp.float32, smallest / len(shards), largest / len(shards))
        factor_of = factor_of * jnp.repeat(jnp.exp(steps), dims[position] // blocks).reshape((-1,) + (1,) * (len(dims) - 1 - position))
    return factor_of


def normal_values(rng, extent, scale, limit, cuts=(), held_as=jnp.bfloat16):
    array = scale * jax.random.normal(rng, extent, jnp.float32)
    if cuts:
        array = array * block_levels(rng, extent, cuts, -0.22, 0.18)
    return jnp.clip(array, -limit, limit).astype(held_as)


def setup_inputs(seed: int = 0) -> dict:
    arg_keys = jax.random.split(jax.random.key(seed), 5)
    return {
        "integrals": normal_values(arg_keys[0], (NT, TILE, V), V ** -0.5, 0.21875, ((0, 32),)),
        "amplitudes": normal_values(arg_keys[1], (IRREPS, V, PP), 1.0, 6.0, ((1, 4), (2, 8))),
        "residual_in": normal_values(arg_keys[2], (NT, TILE, PP), 1.0, 6.0, ((0, 32),)),
        "tile_irrep": draw_tile_irrep(jax.random.fold_in(arg_keys[4], 71), 0),
    }


def reference(integrals, amplitudes, residual_in, tile_irrep):
    def one_tile(operands):
        block, previous, irrep = operands
        chosen = lax.dynamic_index_in_dim(amplitudes, irrep, 0, keepdims=False)
        ladder = jnp.dot(block, chosen, preferred_element_type=jnp.float32)
        return (previous.astype(jnp.float32) + ladder).astype(jnp.bfloat16)

    return lax.map(one_tile, (integrals, residual_in, tile_irrep))
```

```python
import functools

import jax
import jax.numpy as jnp
from jax import lax
from jax.experimental import pallas as pl
from jax.experimental.pallas import tpu as pltpu
from jax.sharding import PartitionSpec as P

MESH = pl.DeviceIdType.MESH
PARTS = 2


def gathered_plan(integrals, amplitudes, residual_in, tile_irrep):
    tile_dev = integrals.shape[0]
    first_tile = (lax.axis_index("tile") * lax.axis_size("bulk") + lax.axis_index("bulk")) * tile_dev
    local_irrep = lax.dynamic_slice_in_dim(tile_irrep, first_tile, tile_dev, 0)
    whole_cd = lax.all_gather(amplitudes, "bulk", axis=1, tiled=True)
    picked = jnp.take(lax.all_gather(whole_cd, "tile", axis=2, tiled=True), local_irrep, axis=0)
    product = jnp.einsum("trc,tcp->trp", integrals, picked, preferred_element_type=jnp.float32)
    return (residual_in.astype(jnp.float32) + product).astype(jnp.bfloat16)


def kernel(rows, bulk, slots, parts, irrep_ref, amp_hbm, int_hbm, res_hbm, out_ref, *scratch):
    cols = rows // 2
    offsets = [0] + [s * d for d in range(1, bulk) for s in (-1, 1)]
    chunks = len(offsets)
    (amp, ints, res, whole), scratch = scratch[:4], scratch[4:]
    held = [[None] * parts] + [list(scratch[i * parts:(i + 1) * parts]) for i in range(chunks - 1)]
    scratch = scratch[(chunks - 1) * parts:]
    picked = [list(scratch[i * parts:(i + 1) * parts]) for i in range(chunks)]
    (z_send, z_recv, c_send, c_recv, p_send, p_recv, local_sem) = scratch[chunks * parts:]
    tiles = ints.shape[0]
    irreps, depth, width = amp.shape
    piece = depth // parts
    me, at = lax.axis_index("tile"), lax.axis_index("bulk")
    col, core = me // 2, me % 2
    partner = col * 2 + (1 - core)

    amp_copy = pltpu.make_async_copy(amp_hbm, amp, local_sem.at[0])
    int_copy = pltpu.make_async_copy(int_hbm, ints, local_sem.at[1])
    res_copy = pltpu.make_async_copy(res_hbm, res, local_sem.at[2])
    amp_copy.start()

    barrier = pltpu.get_barrier_semaphore()
    pl.semaphore_signal(barrier, inc=1, device_id=(partner, at), device_id_type=MESH)
    for j in range(1, cols):
        pl.semaphore_signal(barrier, inc=1, device_id=(lax.rem(col + j, cols) * 2 + core, at), device_id_type=MESH)

    @pl.when(at > 0)
    def _():
        pl.semaphore_signal(barrier, inc=1, device_id=(me, at - 1), device_id_type=MESH)

    @pl.when(at < bulk - 1)
    def _():
        pl.semaphore_signal(barrier, inc=1, device_id=(me, at + 1), device_id_type=MESH)

    int_copy.start()
    res_copy.start()
    pl.semaphore_wait(barrier, cols + (at > 0).astype(jnp.int32) + (at < bulk - 1).astype(jnp.int32))

    amp_copy.wait()

    def block(c, p):
        if c == 0:
            return amp.at[:, pl.ds(p * piece, piece), :]
        return held[c][p]

    def line(c, p, step):
        there = offsets.index(offsets[c] - step)
        way = 0 if step > 0 else 1
        return pltpu.make_async_remote_copy(
            src_ref=block(c, p), dst_ref=held[there][p], send_sem=z_send.at[way, c, p],
            recv_sem=z_recv.at[there, p], device_id=(me, at + step), device_id_type=MESH)

    def line_in(c, p):
        return pltpu.make_async_remote_copy(
            src_ref=held[c][p], dst_ref=held[c][p], send_sem=z_send.at[0, c, p],
            recv_sem=z_recv.at[c, p], device_id=(partner, at), device_id_type=MESH)

    def slab(c, p, row):
        first = pl.multiple_of((at + offsets[c]) * depth + p * piece, 16)
        return whole.at[:, pl.ds(first, piece), pl.ds(pl.multiple_of(row * width, 128), width)]

    def across(c, p, j):
        return pltpu.make_async_remote_copy(
            src_ref=picked[c][p].at[j - 1], dst_ref=slab(c, p, me), send_sem=c_send.at[c, p, j],
            recv_sem=c_recv.at[c, p, j], device_id=(lax.rem(col + j, cols) * 2 + core, at), device_id_type=MESH)

    def over(c, p, j, side):
        row = lax.rem(col - j + cols, cols) * 2 + side
        return pltpu.make_async_remote_copy(
            src_ref=slab(c, p, row), dst_ref=slab(c, p, row), send_sem=p_send.at[c, p, j],
            recv_sem=p_recv.at[c, p, j], device_id=(partner, at), device_id_type=MESH)

    def wanted(column):
        low = (2 * column * bulk + at) * tiles
        high = ((2 * column + 1) * bulk + at) * tiles + tiles - 1
        spots = [low, high] if slots == 2 else [low, low + tiles - 1, high]
        return [irrep_ref[s] for s in spots]

    def present(c):
        src = at + offsets[c]
        return jnp.logical_and(src >= 0, src < bulk)

    def relay(c, p):
        if offsets[c] <= 0:
            @pl.when(at < bulk - 1)
            def _():
                line(c, p, 1).start()
        if offsets[c] >= 0:
            @pl.when(at > 0)
            def _():
                line(c, p, -1).start()

    def relay_done(c, p):
        if offsets[c] <= 0 and offsets[c] - 1 > -bulk:
            @pl.when(at < bulk - 1)
            def _():
                line(c, p, 1).wait_send()
        if offsets[c] >= 0 and offsets[c] + 1 < bulk:
            @pl.when(at > 0)
            def _():
                line(c, p, -1).wait_send()

    def spread(c, p):
        src = amp if c == 0 else held[c][p]
        lanes = pl.ds(p * piece, piece) if c == 0 else slice(None)
        for j in range(1, cols):
            for s, g in enumerate(wanted(lax.rem(col + j, cols))):
                picked[c][p][j - 1, s] = src[g, lanes, :]
            across(c, p, j).start()
        first = pl.multiple_of((at + offsets[c]) * depth + p * piece, 16)
        for s, g in enumerate(wanted(col)):
            whole[s, pl.ds(first, piece), pl.ds(pl.multiple_of(me * width, 128), width)] = src[g, lanes, :]
        over(c, p, 0, core).start()

    def forward(c, p):
        for j in range(1, cols):
            across_in = pltpu.make_async_remote_copy(
                src_ref=slab(c, p, lax.rem(col - j + cols, cols) * 2 + core),
                dst_ref=slab(c, p, lax.rem(col - j + cols, cols) * 2 + core),
                send_sem=c_send.at[c, p, j], recv_sem=c_recv.at[c, p, j],
                device_id=(partner, at), device_id_type=MESH)
            across_in.wait_recv()
            over(c, p, j, core).start()

    for p in range(parts):
        relay(0, p)
    for p in range(parts):
        spread(0, p)
    groups = [[(0, p) for p in range(parts)]]
    for d in range(1, bulk):
        groups.append([(c, p) for p in range(parts) for c in (2 * d - 1, 2 * d)])
    for d in range(1, bulk):
        for c, p in groups[d]:
            @pl.when(present(c))
            def _():
                line_in(c, p).wait_recv()
                if abs(offsets[c]) < bulk - 1:
                    relay(c, p)
                spread(c, p)
        for c, p in groups[d - 1]:
            @pl.when(present(c))
            def _():
                forward(c, p)
    for c, p in groups[bulk - 1]:
        @pl.when(present(c))
        def _():
            forward(c, p)
    int_copy.wait()
    res_copy.wait()
    for group in groups:
        for c, p in group:
            @pl.when(present(c))
            def _():
                for j in range(cols):
                    over(c, p, j, 1 - core).wait_recv()

    mine = wanted(col)
    first_tile = (me * bulk + at) * tiles
    columns = whole.shape[2]
    block_n = 256 if columns % 256 == 0 else 128

    for t in range(tiles):
        irrep = irrep_ref[first_tile + t]
        slot = (irrep > mine[0]).astype(jnp.int32)
        for s in mine[1:-1]:
            slot = slot + (irrep > s).astype(jnp.int32)

        @pl.loop(0, columns // block_n)
        def _(n):
            span = pl.ds(pl.multiple_of(n * block_n, block_n), block_n)
            ladder = jnp.dot(ints[t], whole[slot, :, span], preferred_element_type=jnp.float32)
            out_ref[t, :, span] = (res[t, :, span].astype(jnp.float32) + ladder).astype(jnp.bfloat16)

    for group in groups:
        for c, p in group:
            @pl.when(present(c))
            def _():
                for j in range(cols):
                    over(c, p, j, core).wait_send()
                for j in range(1, cols):
                    across(c, p, j).wait_send()
                relay_done(c, p)

def call(rows, bulk, slots, integrals, amplitudes, residual_in, tile_irrep):
    irreps, depth, width = amplitudes.shape
    parts = PARTS if depth % (16 * PARTS) == 0 else 1
    chunks = 2 * bulk - 1
    cols = rows // 2
    any_space = pl.BlockSpec(memory_space=pl.ANY)
    return pl.pallas_call(
        functools.partial(kernel, rows, bulk, slots, parts),
        out_shape=jax.ShapeDtypeStruct(residual_in.shape, residual_in.dtype),
        in_specs=[pl.BlockSpec(memory_space=pltpu.SMEM), any_space, any_space, any_space],
        out_specs=pl.BlockSpec(memory_space=pltpu.VMEM),
        scratch_shapes=[
            pltpu.VMEM(amplitudes.shape, amplitudes.dtype),
            pltpu.VMEM(integrals.shape, integrals.dtype),
            pltpu.VMEM(residual_in.shape, residual_in.dtype),
            pltpu.VMEM((slots, depth * bulk, width * rows), amplitudes.dtype),
            *[pltpu.VMEM((irreps, depth // parts, width), amplitudes.dtype)] * ((chunks - 1) * parts),
            *[pltpu.VMEM((cols - 1, slots, depth // parts, width), amplitudes.dtype)] * (chunks * parts),
            pltpu.SemaphoreType.DMA((2, chunks, parts)),
            pltpu.SemaphoreType.DMA((chunks, parts)),
            pltpu.SemaphoreType.DMA((chunks, parts, cols)),
            pltpu.SemaphoreType.DMA((chunks, parts, cols)),
            pltpu.SemaphoreType.DMA((chunks, parts, cols)),
            pltpu.SemaphoreType.DMA((chunks, parts, cols)),
            pltpu.SemaphoreType.DMA((3,)),
        ],
        compiler_params=pltpu.CompilerParams(collective_id=slots, has_side_effects=True),
    )(tile_irrep, amplitudes, integrals, residual_in)


def local(rows, bulk, integrals, amplitudes, residual_in, tile_irrep):
    depth, width = amplitudes.shape[1:]
    if rows % 2 or rows < 4 or bulk < 2 or depth % 16 or width % 128:
        return gathered_plan(integrals, amplitudes, residual_in, tile_irrep)
    ends = tile_irrep.reshape(rows // 2, 2, bulk, integrals.shape[0])
    low, high = ends[:, 0, :, 0], ends[:, 1, :, -1]
    mid = ends[:, 0, :, -1]
    mid_too = ends[:, 1, :, 0]
    third = jnp.any(((mid != low) & (mid != high)) | ((mid_too != low) & (mid_too != high)))
    return lax.cond(
        third,
        functools.partial(call, rows, bulk, 3),
        functools.partial(call, rows, bulk, 2),
        integrals, amplitudes, residual_in, tile_irrep)


def solution(mesh):
    return jax.shard_map(
        functools.partial(local, mesh.shape["tile"], mesh.shape["bulk"]),
        mesh=mesh,
        in_specs=(
            P(("tile", "bulk"), None, None),
            P(None, "bulk", "tile"),
            P(("tile", "bulk"), None, None),
            P(),
        ),
        out_specs=P(("tile", "bulk"), None, None),
        check_vma=False,
    )
```

```python
import functools

import jax
import jax.numpy as jnp
from jax import lax
from jax.experimental import pallas as pl
from jax.experimental.pallas import tpu as pltpu
from jax.sharding import PartitionSpec as P

MESH = pl.DeviceIdType.MESH
PARTS = 2


def gathered_plan(integrals, amplitudes, residual_in, tile_irrep):
    tile_dev = integrals.shape[0]
    first_tile = (lax.axis_index("tile") * lax.axis_size("bulk") + lax.axis_index("bulk")) * tile_dev
    local_irrep = lax.dynamic_slice_in_dim(tile_irrep, first_tile, tile_dev, 0)
    whole_cd = lax.all_gather(amplitudes, "bulk", axis=1, tiled=True)
    picked = jnp.take(lax.all_gather(whole_cd, "tile", axis=2, tiled=True), local_irrep, axis=0)
    product = jnp.einsum("trc,tcp->trp", integrals, picked, preferred_element_type=jnp.float32)
    return (residual_in.astype(jnp.float32) + product).astype(jnp.bfloat16)


def kernel(rows, bulk, slots, parts, irrep_ref, amp_hbm, int_hbm, res_hbm, out_ref, *scratch):
    cols = rows // 2
    offsets = [0] + [s * d for d in range(1, bulk) for s in (-1, 1)]
    chunks = len(offsets)
    (amp, ints, res, whole), scratch = scratch[:4], scratch[4:]
    held = [[None] * parts] + [list(scratch[i * parts:(i + 1) * parts]) for i in range(chunks - 1)]
    scratch = scratch[(chunks - 1) * parts:]
    picked = [list(scratch[i * parts:(i + 1) * parts]) for i in range(chunks)]
    (z_send, z_recv, c_send, c_recv, p_send, p_recv, local_sem) = scratch[chunks * parts:]
    tiles = ints.shape[0]
    irreps, depth, width = amp.shape
    piece = depth // parts
    me, at = lax.axis_index("tile"), lax.axis_index("bulk")
    col, core = me // 2, me % 2
    partner = col * 2 + (1 - core)

    amp_copy = pltpu.make_async_copy(amp_hbm, amp, local_sem.at[0])
    int_copy = pltpu.make_async_copy(int_hbm, ints, local_sem.at[1])
    res_copy = pltpu.make_async_copy(res_hbm, res, local_sem.at[2])
    amp_copy.start()

    barrier = pltpu.get_barrier_semaphore()
    pl.semaphore_signal(barrier, inc=1, device_id=(partner, at), device_id_type=MESH)
    for j in range(1, cols):
        pl.semaphore_signal(barrier, inc=1, device_id=(lax.rem(col + j, cols) * 2 + core, at), device_id_type=MESH)

    @pl.when(at > 0)
    def _():
        pl.semaphore_signal(barrier, inc=1, device_id=(me, at - 1), device_id_type=MESH)

    @pl.when(at < bulk - 1)
    def _():
        pl.semaphore_signal(barrier, inc=1, device_id=(me, at + 1), device_id_type=MESH)

    int_copy.start()
    res_copy.start()
    pl.semaphore_wait(barrier, cols + (at > 0).astype(jnp.int32) + (at < bulk - 1).astype(jnp.int32))

    amp_copy.wait()

    def block(c, p):
        if c == 0:
            return amp.at[:, pl.ds(p * piece, piece), :]
        return held[c][p]

    def line(c, p, step):
        there = offsets.index(offsets[c] - step)
        way = 0 if step > 0 else 1
        return pltpu.make_async_remote_copy(
            src_ref=block(c, p), dst_ref=held[there][p], send_sem=z_send.at[way, c, p],
            recv_sem=z_recv.at[there, p], device_id=(me, at + step), device_id_type=MESH)

    def line_in(c, p):
        return pltpu.make_async_remote_copy(
            src_ref=held[c][p], dst_ref=held[c][p], send_sem=z_send.at[0, c, p],
            recv_sem=z_recv.at[c, p], device_id=(partner, at), device_id_type=MESH)

    def slab(c, p, row):
        first = pl.multiple_of((at + offsets[c]) * depth + p * piece, 16)
        return whole.at[:, pl.ds(first, piece), pl.ds(pl.multiple_of(row * width, 128), width)]

    def across(c, p, j):
        return pltpu.make_async_remote_copy(
            src_ref=picked[c][p].at[j - 1], dst_ref=slab(c, p, me), send_sem=c_send.at[c, p, j],
            recv_sem=c_recv.at[c, p, j], device_id=(lax.rem(col + j, cols) * 2 + core, at), device_id_type=MESH)

    def over(c, p, j, side):
        row = lax.rem(col - j + cols, cols) * 2 + side
        return pltpu.make_async_remote_copy(
            src_ref=slab(c, p, row), dst_ref=slab(c, p, row), send_sem=p_send.at[c, p, j],
            recv_sem=p_recv.at[c, p, j], device_id=(partner, at), device_id_type=MESH)

    def wanted(column):
        low = (2 * column * bulk + at) * tiles
        high = ((2 * column + 1) * bulk + at) * tiles + tiles - 1
        spots = [low, high] if slots == 2 else [low, low + tiles - 1, high]
        return [irrep_ref[s] for s in spots]

    def present(c):
        src = at + offsets[c]
        return jnp.logical_and(src >= 0, src < bulk)

    def relay(c, p):
        if offsets[c] <= 0:
            @pl.when(at < bulk - 1)
            def _():
                line(c, p, 1).start()
        if offsets[c] >= 0:
            @pl.when(at > 0)
            def _():
                line(c, p, -1).start()

    def relay_done(c, p):
        if offsets[c] <= 0 and offsets[c] - 1 > -bulk:
            @pl.when(at < bulk - 1)
            def _():
                line(c, p, 1).wait_send()
        if offsets[c] >= 0 and offsets[c] + 1 < bulk:
            @pl.when(at > 0)
            def _():
                line(c, p, -1).wait_send()

    def spread(c, p):
        src = amp if c == 0 else held[c][p]
        lanes = pl.ds(p * piece, piece) if c == 0 else slice(None)
        for j in range(1, cols):
            for s, g in enumerate(wanted(lax.rem(col + j, cols))):
                picked[c][p][j - 1, s] = src[g, lanes, :]
            across(c, p, j).start()
        first = pl.multiple_of((at + offsets[c]) * depth + p * piece, 16)
        for s, g in enumerate(wanted(col)):
            whole[s, pl.ds(first, piece), pl.ds(pl.multiple_of(me * width, 128), width)] = src[g, lanes, :]
        over(c, p, 0, core).start()

    def forward(c, p):
        for j in range(1, cols):
            across_in = pltpu.make_async_remote_copy(
                src_ref=slab(c, p, lax.rem(col - j + cols, cols) * 2 + core),
                dst_ref=slab(c, p, lax.rem(col - j + cols, cols) * 2 + core),
                send_sem=c_send.at[c, p, j], recv_sem=c_recv.at[c, p, j],
                device_id=(partner, at), device_id_type=MESH)
            across_in.wait_recv()
            over(c, p, j, core).start()

    for p in range(parts):
        relay(0, p)
    for p in range(parts):
        spread(0, p)
    groups = [[(0, p) for p in range(parts)]]
    for d in range(1, bulk):
        groups.append([(c, p) for p in range(parts) for c in (2 * d - 1, 2 * d)])
    for d in range(1, bulk):
        for c, p in groups[d]:
            @pl.when(present(c))
            def _():
                line_in(c, p).wait_recv()
                if abs(offsets[c]) < bulk - 1:
                    relay(c, p)
                spread(c, p)
        for c, p in groups[d - 1]:
            @pl.when(present(c))
            def _():
                forward(c, p)
    for c, p in groups[bulk - 1]:
        @pl.when(present(c))
        def _():
            forward(c, p)
    int_copy.wait()
    res_copy.wait()
    for group in groups:
        for c, p in group:
            @pl.when(present(c))
            def _():
                for j in range(cols):
                    over(c, p, j, 1 - core).wait_recv()

    mine = wanted(col)
    first_tile = (me * bulk + at) * tiles
    columns = whole.shape[2]
    block_n = 512 if columns % 512 == 0 else 128

    for t in range(tiles):
        irrep = irrep_ref[first_tile + t]
        slot = (irrep > mine[0]).astype(jnp.int32)
        for s in mine[1:-1]:
            slot = slot + (irrep > s).astype(jnp.int32)

        @pl.loop(0, columns // block_n)
        def _(n):
            span = pl.ds(pl.multiple_of(n * block_n, block_n), block_n)
            ladder = jnp.dot(ints[t], whole[slot, :, span], preferred_element_type=jnp.float32)
            out_ref[t, :, span] = (res[t, :, span].astype(jnp.float32) + ladder).astype(jnp.bfloat16)

    for group in groups:
        for c, p in group:
            @pl.when(present(c))
            def _():
                for j in range(cols):
                    over(c, p, j, core).wait_send()
                for j in range(1, cols):
                    across(c, p, j).wait_send()
                relay_done(c, p)

def call(rows, bulk, slots, integrals, amplitudes, residual_in, tile_irrep):
    irreps, depth, width = amplitudes.shape
    parts = PARTS if depth % (16 * PARTS) == 0 else 1
    chunks = 2 * bulk - 1
    cols = rows // 2
    any_space = pl.BlockSpec(memory_space=pl.ANY)
    return pl.pallas_call(
        functools.partial(kernel, rows, bulk, slots, parts),
        out_shape=jax.ShapeDtypeStruct(residual_in.shape, residual_in.dtype),
        in_specs=[pl.BlockSpec(memory_space=pltpu.SMEM), any_space, any_space, any_space],
        out_specs=pl.BlockSpec(memory_space=pltpu.VMEM),
        scratch_shapes=[
            pltpu.VMEM(amplitudes.shape, amplitudes.dtype),
            pltpu.VMEM(integrals.shape, integrals.dtype),
            pltpu.VMEM(residual_in.shape, residual_in.dtype),
            pltpu.VMEM((slots, depth * bulk, width * rows), amplitudes.dtype),
            *[pltpu.VMEM((irreps, depth // parts, width), amplitudes.dtype)] * ((chunks - 1) * parts),
            *[pltpu.VMEM((cols - 1, slots, depth // parts, width), amplitudes.dtype)] * (chunks * parts),
            pltpu.SemaphoreType.DMA((2, chunks, parts)),
            pltpu.SemaphoreType.DMA((chunks, parts)),
            pltpu.SemaphoreType.DMA((chunks, parts, cols)),
            pltpu.SemaphoreType.DMA((chunks, parts, cols)),
            pltpu.SemaphoreType.DMA((chunks, parts, cols)),
            pltpu.SemaphoreType.DMA((chunks, parts, cols)),
            pltpu.SemaphoreType.DMA((3,)),
        ],
        compiler_params=pltpu.CompilerParams(collective_id=slots, has_side_effects=True),
    )(tile_irrep, amplitudes, integrals, residual_in)


def local(rows, bulk, integrals, amplitudes, residual_in, tile_irrep):
    depth, width = amplitudes.shape[1:]
    if rows % 2 or rows < 4 or bulk < 2 or depth % 16 or width % 128:
        return gathered_plan(integrals, amplitudes, residual_in, tile_irrep)
    ends = tile_irrep.reshape(rows // 2, 2, bulk, integrals.shape[0])
    low, high = ends[:, 0, :, 0], ends[:, 1, :, -1]
    mid = ends[:, 0, :, -1]
    mid_too = ends[:, 1, :, 0]
    third = jnp.any(((mid != low) & (mid != high)) | ((mid_too != low) & (mid_too != high)))
    return lax.cond(
        third,
        functools.partial(call, rows, bulk, 3),
        functools.partial(call, rows, bulk, 2),
        integrals, amplitudes, residual_in, tile_irrep)


def solution(mesh):
    return jax.shard_map(
        functools.partial(local, mesh.shape["tile"], mesh.shape["bulk"]),
        mesh=mesh,
        in_specs=(
            P(("tile", "bulk"), None, None),
            P(None, "bulk", "tile"),
            P(("tile", "bulk"), None, None),
            P(),
        ),
        out_specs=P(("tile", "bulk"), None, None),
        check_vma=False,
    )
```
